256 devices in a mesh: tm: 16 (over x, z_lo), py: 4 (over y), pz: 4 (over z_hi, core).
Axes of the slice: x: 4, y: 4, z: 8 (z_hi: 2, z_lo: 4; z = z_hi * 4 + z_lo), core: 2. Of those that a mesh axis runs over, the one named last changes fastest.
Arguments:
- start_states: float32 [16, 3, 128, 8, 16, 128], P('tm', None, None, None, ('py', 'pz')), may hold values from -6 to 6
Outputs:
- new_states: float32 [16, 3, 128, 8, 16, 128], P('tm', None, None, None, ('py', 'pz'))
The draws below stay inside these ranges and needn't reach their ends.
All inputs are finite; a program needn't handle non-finite values.
Results may differ from the reference program's by a relative error of at most 0.0001.
Values sent between devices are 32-bit elements; how exact they have to be, the bound alone decides.
No kernel may reach another device: no remote copies, remote signals or barrier semaphores. Data moves between devices by JAX's collectives and lax.ppermute only.
A program may use at most 128 MiB of HBM per device.

```python
import jax
import jax.numpy as jnp
from jax import lax

N = 128
M = 64
PEN = 16
SLICES = 16


def shard_levels(rng, shape, shards, least, high):
    level = 1.0
    for dim, shards_of in shards:
        draws = jax.random.uniform(jax.random.fold_in(jax.random.fold_in(rng, 6), dim), (shards_of,), jnp.float32, least / len(shards), high / len(shards))
        level = level * jnp.repeat(jnp.exp(draws), shape[dim] // shards_of).reshape((-1,) + (1,) * (len(shape) - 1 - dim))
    return level


def bell_draw(rng, shape, width, most, cuts=(), kind=jnp.bfloat16):
    entries = width * jax.random.normal(rng, shape, jnp.float32)
    if cuts:
        entries = entries * shard_levels(rng, shape, cuts, -0.22, 0.18)
    return jnp.clip(entries, -most, most).astype(kind)


def setup_inputs(seed: int = 0) -> dict:
    arg_keys = jax.random.split(jax.random.key(seed), 2)
    return {
        "start_states": bell_draw(arg_keys[0], (SLICES, 3, N, N // PEN, PEN, N), 1.0, 6.0, ((0, 16), (4, 16)), jnp.float32),
    }


viscosity = 0.03
time_step = 0.004


def signed_wave(length):
    places = jnp.arange(length, dtype=jnp.int32)
    return jnp.where(places < length // 2, places, places - length).astype(jnp.float32)


def wavenumbers(retained):
    wave_x = signed_wave(retained)[:, None, None]
    wave_y = signed_wave(retained)[None, :, None]
    wave_z = jnp.arange(retained // 2, dtype=jnp.int32).astype(jnp.float32)[None, None, :]
    return wave_x, wave_y, wave_z


def vorticity(coeffs, wavegrid):
    wave_x, wave_y, wave_z = wavegrid
    along_x = 1j * (wave_y * coeffs[2] - wave_z * coeffs[1])
    along_y = 1j * (wave_z * coeffs[0] - wave_x * coeffs[2])
    along_z = 1j * (wave_x * coeffs[1] - wave_y * coeffs[0])
    return jnp.stack([along_x, along_y, along_z])


def project(coeffs, wavegrid):
    wave_x, wave_y, wave_z = wavegrid
    squared = wave_x * wave_x + wave_y * wave_y + wave_z * wave_z
    divergence = (wave_x * coeffs[0] + wave_y * coeffs[1] + wave_z * coeffs[2]) / jnp.maximum(squared, 1.0)
    return jnp.stack([coeffs[0] - wave_x * divergence, coeffs[1] - wave_y * divergence, coeffs[2] - wave_z * divergence])


def cross_product(first_field, second_field):
    return jnp.stack([
        first_field[1] * second_field[2] - first_field[2] * second_field[1],
        first_field[2] * second_field[0] - first_field[0] * second_field[2],
        first_field[0] * second_field[1] - first_field[1] * second_field[0],
    ])


def widen(coeffs, extent, contracted):
    length = coeffs.shape[contracted]
    halfway = length // 2
    low_part = lax.slice_in_dim(coeffs, 0, halfway, axis=contracted)
    high_part = lax.slice_in_dim(coeffs, halfway, length, axis=contracted)
    filler_shape = list(coeffs.shape)
    filler_shape[contracted] = extent - length
    return jnp.concatenate([low_part, jnp.zeros(filler_shape, coeffs.dtype), high_part], axis=contracted)


def narrow(coeffs, kept, contracted):
    length = coeffs.shape[contracted]
    halfway = kept // 2
    low_part = lax.slice_in_dim(coeffs, 0, halfway, axis=contracted)
    high_part = lax.slice_in_dim(coeffs, length - halfway, length, axis=contracted)
    return jnp.concatenate([low_part, high_part], axis=contracted)


def widen_last(coeffs, columns):
    filler_shape = list(coeffs.shape)
    filler_shape[3] = columns - coeffs.shape[3]
    return jnp.concatenate([coeffs, jnp.zeros(filler_shape, coeffs.dtype)], axis=3)


def to_physical(coeffs, extent):
    retained = coeffs.shape[1]
    spread = widen(widen(coeffs, extent, 1), extent, 2)
    spread = widen_last(spread, extent // 2 + 1)
    spread = jnp.fft.ifft(spread, axis=1)
    spread = jnp.fft.ifft(spread, axis=2)
    constant_column = jnp.real(spread[..., :1]).astype(spread.dtype)
    spread = jnp.concatenate([constant_column, spread[..., 1:]], axis=3)
    return jnp.fft.irfft(spread, n=extent, axis=3) * (extent ** 3 / retained ** 1.5)


def to_spectral(fields, retained):
    extent = fields.shape[-1]
    spectrum = jnp.fft.rfftn(fields, axes=(1, 2, 3))
    spectrum = narrow(narrow(spectrum, retained, 1), retained, 2)[..., : retained // 2]
    return spectrum * (retained ** 1.5 / extent ** 3)


def restrict(coeffs, kept):
    return narrow(narrow(coeffs, kept, 1), kept, 2)[..., : kept // 2]


def prolong(coeffs, retained):
    wider = widen(widen(coeffs, retained, 1), retained, 2)
    return widen_last(wider, retained // 2)


def advance(coeffs):
    retained = coeffs.shape[1]
    extent = 3 * retained // 2
    wavegrid = wavenumbers(retained)
    fields = to_physical(jnp.concatenate([coeffs, vorticity(coeffs, wavegrid)], axis=0), extent)
    product = cross_product(fields[:3], fields[3:])
    nonlinear = to_spectral(product, retained)
    wave_x, wave_y, wave_z = wavegrid
    squared = wave_x * wave_x + wave_y * wave_y + wave_z * wave_z
    damping = jnp.exp(-viscosity * time_step * squared)
    return damping * (coeffs + time_step * project(nonlinear, wavegrid))


def pack(coeffs):
    merged = jnp.concatenate([jnp.real(coeffs), jnp.imag(coeffs)], axis=-1).astype(jnp.float32)
    return merged.reshape(3, N, N // PEN, PEN, N)


def unpack(stored):
    merged = stored.reshape(3, N, N, N)
    return merged[..., : N // 2] + 1j * merged[..., N // 2:]


def reference(start_states):
    slices = start_states.shape[0]
    fine_ends = []
    corrections = []
    first_state = None
    for slice_number in range(slices):
        spectral_state = project(unpack(start_states[slice_number]), wavenumbers(N))
        if slice_number == 0:
            first_state = spectral_state
        fine_end = advance(spectral_state)
        coarse_next = advance(restrict(spectral_state, M))
        fine_ends.append(fine_end)
        corrections.append(restrict(fine_end, M) - coarse_next)
    chained = restrict(fine_ends[0], M)
    packed = [pack(first_state)]
    for slice_number in range(1, slices):
        previous = fine_ends[slice_number - 1]
        upper_band = previous - prolong(restrict(previous, M), N)
        packed.append(pack(prolong(chained, N) + upper_band))
        if slice_number < slices - 1:
            chained = advance(chained) + corrections[slice_number]
    return jnp.stack(packed)
```

```python
from functools import partial
import math

import jax
import jax.numpy as jnp
import numpy as np
from jax import lax
from jax.experimental import pallas as pl
from jax.experimental.pallas import tpu as pltpu
from jax.sharding import Mesh
from jax.sharding import PartitionSpec as P


M = 64


viscosity = 0.03
time_step = 0.004
highest = lax.Precision.HIGH


def shifted(block, axis, distance):
    devices = range(lax.axis_size(axis))
    route = [(i - distance, i) for i in devices if i - distance in devices]
    return lax.ppermute(block, axis, route)


def signed_wave(places, length):
    return jnp.where(places < length // 2, places, places - length)


def rotate(values):
    halfway = values.shape[-1] // 2
    return jnp.concatenate([-values[..., halfway:], values[..., :halfway]], axis=-1)


def trig_pair(outer, inner, extent, factor):
    residue = jnp.mod(outer[:, None] * inner[None, :], extent)
    radians = residue.astype(jnp.float32) * (2.0 * math.pi / extent)
    return (jnp.cos(radians) * factor, jnp.sin(radians) * factor)


def complex_apply(cosine_part, sine_part, values, contracted, direction_sign):
    kernel = jnp.stack(
        [
            jnp.stack([cosine_part, -direction_sign * sine_part]),
            jnp.stack([direction_sign * sine_part, cosine_part]),
        ]
    )
    halfway = values.shape[-1] // 2
    split = values.reshape(values.shape[:-1] + (2, halfway))
    if contracted == 1:
        pattern = "pqok,fkaqh->foaph"
    else:
        pattern = "pqok,flkqh->floph"
    result = jnp.einsum(pattern, kernel, split, precision=highest)
    return result.reshape(result.shape[:-2] + (2 * halfway,))


def inverse_z(extent, retained):
    halfway = retained // 2
    columns = jnp.arange(retained, dtype=jnp.int32)
    harmonic = columns % halfway
    weight = jnp.where(harmonic == 0, 1.0, 2.0) * retained ** (-0.5)
    residue = jnp.mod(harmonic[:, None] * jnp.arange(extent, dtype=jnp.int32)[None, :], extent)
    radians = residue.astype(jnp.float32) * (2.0 * math.pi / extent)
    return (
        jnp.where((columns < halfway)[:, None], jnp.cos(radians), -jnp.sin(radians))
        * weight[:, None]
    )


def forward_z(extent, retained):
    halfway = retained // 2
    columns = jnp.arange(retained, dtype=jnp.int32)
    harmonic = columns % halfway
    residue = jnp.mod(jnp.arange(extent, dtype=jnp.int32)[:, None] * harmonic[None, :], extent)
    radians = residue.astype(jnp.float32) * (2.0 * math.pi / extent)
    return jnp.where((columns < halfway)[None, :], jnp.cos(radians), -jnp.sin(radians)) * (
        math.sqrt(retained) / extent
    )


def exchange(block, split_dim, concat_dim):
    return lax.all_to_all(
        block, ("y", "zh", "core"), split_axis=split_dim, concat_axis=concat_dim, tiled=True
    )


def wave_y_places(retained, groups):
    local_rows = retained // groups
    places = jnp.arange(retained, dtype=jnp.int32)
    return signed_wave(places % local_rows * groups + places // local_rows, retained)


def inverse_tail(portion, extent, groups):
    retained = portion.shape[2]
    points = jnp.arange(extent, dtype=jnp.int32)
    wave_y = wave_y_places(retained, groups)
    cosine_part, sine_part = trig_pair(points, wave_y, extent, retained ** (-0.5))
    along_y = complex_apply(cosine_part, sine_part, portion, 2, 1.0)
    return jnp.einsum("flyr,rz->flyz", along_y, inverse_z(extent, retained), precision=highest)


def forward_tail(portion, retained):
    extent = portion.shape[1]
    points = jnp.arange(extent, dtype=jnp.int32)
    wave_x = signed_wave(jnp.arange(retained, dtype=jnp.int32), retained)
    cosine_part, sine_part = trig_pair(wave_x, points, extent, math.sqrt(retained) / extent)
    return complex_apply(cosine_part, sine_part, portion, 1, -1.0)


def spread_x(coeffs, wavegrid, extent):
    wave_x = wavegrid[0]
    retained = coeffs.shape[1]
    points = jnp.arange(extent, dtype=jnp.int32)
    wave_rows = signed_wave(jnp.arange(retained, dtype=jnp.int32), retained)
    cosine_part, sine_part = trig_pair(points, wave_rows, extent, retained ** (-0.5))
    moved = complex_apply(cosine_part, sine_part, coeffs, 1, 1.0)
    slopes = complex_apply(cosine_part, sine_part, wave_x * coeffs[1:3], 1, 1.0)
    return moved, slopes


def to_physical(moved, slopes, wavegrid, extent, groups):
    wave_z = wavegrid[2]
    retained = moved.shape[2]
    all_y = wave_y_places(retained, groups).astype(jnp.float32)[None, :, None]
    velocity = inverse_tail(moved, extent, groups)
    curl_x = rotate(all_y * moved[2] - wave_z * moved[1])
    curl_y = rotate(wave_z * moved[0] - slopes[1])
    curl_z = rotate(slopes[0] - all_y * moved[0])
    return velocity, inverse_tail(jnp.stack([curl_x, curl_y, curl_z]), extent, groups)


def along_planes(fields, retained, groups):
    extent = fields.shape[-1]
    along_z = jnp.einsum("flyz,zr->flyr", fields, forward_z(extent, retained), precision=highest)
    wave_y = wave_y_places(retained, groups)
    cosine_part, sine_part = trig_pair(
        wave_y, jnp.arange(extent, dtype=jnp.int32), extent, math.sqrt(retained) / extent
    )
    return complex_apply(cosine_part, sine_part, along_z, 2, -1.0)


def wave_grid(retained, layout):
    _, _, groups, member = layout
    places = jnp.arange(retained, dtype=jnp.int32)
    wave_x = signed_wave(places, retained).astype(jnp.float32)[:, None, None]
    local_places = jnp.arange(retained // groups, dtype=jnp.int32)
    wave_y = signed_wave(local_places * groups + member, retained).astype(jnp.float32)[
        None, :, None
    ]
    wave_z = (places % (retained // 2)).astype(jnp.float32)[None, None, :]
    return (wave_x, wave_y, wave_z)


def project(coeffs, wavegrid):
    wave_x, wave_y, wave_z = wavegrid
    squared = wave_x * wave_x + wave_y * wave_y + wave_z * wave_z
    divergence = (wave_x * coeffs[0] + wave_y * coeffs[1] + wave_z * coeffs[2]) / jnp.maximum(
        squared, 1.0
    )
    return jnp.stack(
        [
            coeffs[0] - wave_x * divergence,
            coeffs[1] - wave_y * divergence,
            coeffs[2] - wave_z * divergence,
        ]
    )


def cross_parts(first_field, second_field):
    return [
        first_field[1] * second_field[2] - first_field[2] * second_field[1],
        first_field[2] * second_field[0] - first_field[0] * second_field[2],
        first_field[0] * second_field[1] - first_field[1] * second_field[0],
    ]


def advance_both(coeffs, low_states, place, layout):
    groups = layout[2]
    retained = coeffs.shape[1]
    extent = 3 * retained // 2
    wavegrid = wave_grid(retained, layout)
    start, _, move, grid_work, mode_work = chain_steps(place)
    moved, slopes = spread_x(coeffs, wavegrid, extent)
    moved, slopes, low_states = lax.optimization_barrier((moved, slopes, low_states))
    moved, slopes = exchange(moved, 1, 2), exchange(slopes, 1, 2)
    parcels = jnp.concatenate([start(low_states[0]), start(low_states[1])], axis=1)
    moved, slopes, parcels = lax.optimization_barrier((moved, slopes, parcels))
    arrived = move(parcels)
    velocity, curl = to_physical(moved, slopes, wavegrid, extent, groups)
    velocity, curl, arrived = lax.optimization_barrier((velocity, curl, arrived))
    products = [grid_work(arrived[:, :rows_sent]), grid_work(arrived[:, rows_sent:])]
    products = jnp.concatenate(products, axis=1)
    parts = [
        exchange(along_planes(part[None], retained, groups), 2, 1)
        for part in cross_parts(velocity, curl)
    ]
    parts, products = lax.optimization_barrier((parts, products))
    arrived = move(products)
    nonlinear = jnp.concatenate([forward_tail(part, retained) for part in parts])
    wave_x, wave_y, wave_z = wavegrid
    squared = wave_x * wave_x + wave_y * wave_y + wave_z * wave_z
    damping = jnp.exp(-viscosity * time_step * squared)
    fine_end = damping * (coeffs + time_step * project(nonlinear, wavegrid))
    fine_end, arrived = lax.optimization_barrier((fine_end, arrived))
    nothing = jnp.zeros((3, M, 128), jnp.float32)
    first = mode_work(arrived[:, :rows_sent], low_states[0], nothing)[0]
    second = mode_work(arrived[:, rows_sent:], low_states[1], nothing)[0]
    return fine_end, jnp.stack([first, second])


def restrict(coeffs, kept, groups):
    halfway = kept // 2
    retained = coeffs.shape[1]
    rows_kept = jnp.concatenate([coeffs[:, :halfway], coeffs[:, retained - halfway :]], axis=1)
    local_rows = coeffs.shape[2]
    local_kept = kept // groups // 2
    rows_kept = jnp.concatenate(
        [rows_kept[:, :, :local_kept], rows_kept[:, :, local_rows - local_kept :]], axis=2
    )
    columns_half = coeffs.shape[3] // 2
    return jnp.concatenate(
        [rows_kept[..., :halfway], rows_kept[..., columns_half : columns_half + halfway]], axis=3
    )


def shared_modes(retained, groups):
    limit = M // 2
    local_rows = retained // groups
    local_limit = limit // groups
    along_x = jnp.arange(retained, dtype=jnp.int32)
    along_y = jnp.arange(local_rows, dtype=jnp.int32)
    along_z = jnp.arange(retained, dtype=jnp.int32) % (retained // 2)
    keep_x = (along_x < limit) | (along_x >= retained - limit)
    keep_y = (along_y < local_limit) | (along_y >= local_rows - local_limit)
    keep_z = along_z < limit
    return keep_x[:, None, None] & keep_y[None, :, None] & keep_z[None, None, :]


def prolong(coeffs, retained, groups):
    components, kept, local_kept, width = coeffs.shape
    halfway = kept // 2
    zeros_x = jnp.zeros((components, retained - kept, local_kept, width), jnp.float32)
    wider = jnp.concatenate([coeffs[:, :halfway], zeros_x, coeffs[:, halfway:]], axis=1)
    local_rows = retained // groups
    split_rows = local_kept // 2
    zeros_y = jnp.zeros((components, retained, local_rows - local_kept, width), jnp.float32)
    wider = jnp.concatenate([wider[:, :, :split_rows], zeros_y, wider[:, :, split_rows:]], axis=2)
    zeros_z = jnp.zeros((components, retained, local_rows, retained // 2 - halfway), jnp.float32)
    return jnp.concatenate([wider[..., :halfway], zeros_z, wider[..., halfway:], zeros_z], axis=3)


ring = ("x", "y", "core")
peers = 32
planes = 3
rows_sent = 16
grid_side = 3 * M // 2


def two_parts(values):
    high = values.astype(jnp.bfloat16)
    return high, (values - high.astype(jnp.float32)).astype(jnp.bfloat16)


def table_parts(table):
    table = table.astype(np.float32)
    high = table.astype(jnp.bfloat16)
    low = (table - high.astype(np.float32)).astype(jnp.bfloat16)
    return high, low


def left_table(table):
    high, low = table_parts(table)
    return np.concatenate([high, high, low], axis=1)


def from_left(table, values):
    high, low = two_parts(values)
    stacked = jnp.concatenate([high, low, high], axis=0)
    return jnp.dot(table, stacked, preferred_element_type=jnp.float32)


def chain_tables():
    points = np.arange(grid_side)
    step = 2.0 * np.pi / grid_side
    member = np.arange(peers)
    wave_y = member // 8 * 16 + member // 2 % 4 * 4 + member % 2
    wave_y = np.where(wave_y < M // 2, wave_y, wave_y - M)
    angle_y = np.outer(points, wave_y) * step
    lanes = np.arange(128)
    pair = lanes // 64
    half = M // 2
    wave_z = lanes % half
    imaginary = lanes % 64 >= half
    inverse_y = np.concatenate([np.cos(angle_y), np.sin(angle_y)], axis=0) * M**-0.5
    twist = np.outer(points, 2 * pair) * step
    turn_cos, turn_sin = np.cos(twist), np.sin(twist)
    angle_z = np.outer(wave_z, points) * step
    weight = (np.where(wave_z == 0, 1.0, 2.0) * M**-0.5)[:, None]
    plain = np.where(imaginary[:, None], -np.sin(angle_z), np.cos(angle_z)) * weight
    turned = np.where(imaginary[:, None], -np.cos(angle_z), -np.sin(angle_z)) * weight
    inverse_z = np.zeros((256, 128))
    inverse_z[:128, :grid_side] = plain
    inverse_z[128:, :grid_side] = turned
    iz_high, iz_low = table_parts(inverse_z)
    iz_both = np.concatenate([iz_high, iz_low], axis=1)
    scale = M**0.5 / grid_side
    forward_z = np.zeros((128, 256))
    forward_z[:grid_side, :128] = np.where(imaginary[:, None], -np.sin(angle_z), np.cos(angle_z)).T * scale
    forward_z[:grid_side, 128:] = np.where(imaginary[:, None], -np.cos(angle_z), -np.sin(angle_z)).T * scale
    fz_high, fz_low = table_parts(forward_z)
    fz_all = np.concatenate([fz_high, fz_high, fz_low], axis=0)
    forward_y = np.concatenate([np.cos(angle_y.T), np.sin(angle_y.T)], axis=1) * scale
    member_x = np.arange(grid_side)
    wave_x = np.where(np.arange(M) < half, np.arange(M), np.arange(M) - M)
    angle_x = np.outer(wave_x, member_x) * step
    forward_x = np.concatenate([np.cos(angle_x), np.sin(angle_x)], axis=1) * scale
    inverse_x = np.concatenate([np.cos(angle_x.T), np.sin(angle_x.T)], axis=1) * M**-0.5
    lanes_y = np.broadcast_to(wave_y[:, None] + 2 * pair[None, :], (peers, 128))
    lanes_z = np.broadcast_to(wave_z[None, :], (peers, 128))
    return {
        "inverse_y": left_table(inverse_y),
        "turn_cos": turn_cos.astype(np.float32),
        "turn_sin": turn_sin.astype(np.float32),
        "iz_both": iz_both,
        "iz_high": iz_high,
        "fz_all": fz_all,
        "forward_y": left_table(forward_y),
        "forward_x": left_table(forward_x),
        "inverse_x": left_table(inverse_x),
        "lanes_y": lanes_y.astype(np.float32),
        "lanes_z": lanes_z.astype(np.float32),
        "wave_x": np.broadcast_to(wave_x[:, None], (M, 128)).astype(np.float32),
    }


def times_i(values):
    lane = lax.broadcasted_iota(jnp.int32, values.shape, 1)
    ahead = pltpu.roll(values, 96, 1)
    behind = pltpu.roll(values, 32, 1)
    return jnp.where(lane % 64 < 32, -ahead, behind)


def grid_kernel(arrived, iy, tc, ts, iz_both, iz_high, fz_all, fy, ly, lz, sent):
    wave_y, wave_z = ly[...], lz[...]
    turn_cos, turn_sin = tc[...], ts[...]
    for plane in range(planes):
        ux, uy, uz, dy, dz = [arrived[:, plane * 5 + k, :] for k in range(5)]
        wx = times_i(wave_y * uz - wave_z * uy)
        wy = times_i(wave_z * ux) - dz
        wz = dy - times_i(wave_y * ux)
        packed = jnp.concatenate([ux, uy, uz, wx, wy, wz], axis=1)
        along_y = from_left(iy[...], packed)
        pieces = []
        for k in range(6):
            c = along_y[:grid_side, k * 128 : (k + 1) * 128]
            s = along_y[grid_side:, k * 128 : (k + 1) * 128]
            pieces.append(
                jnp.concatenate([turn_cos * c - turn_sin * s, turn_cos * s + turn_sin * c], axis=1)
            )
        high, low = two_parts(jnp.concatenate(pieces, axis=0))
        wide = jnp.dot(high, iz_both[...], preferred_element_type=jnp.float32)
        rest = jnp.dot(low, iz_high[...], preferred_element_type=jnp.float32)
        field = wide[:, :128] + wide[:, 128:] + rest
        f = [field[k * grid_side : (k + 1) * grid_side] for k in range(6)]
        product = jnp.concatenate(
            [
                f[1] * f[5] - f[2] * f[4],
                f[2] * f[3] - f[0] * f[5],
                f[0] * f[4] - f[1] * f[3],
            ],
            axis=0,
        )
        high, low = two_parts(product)
        along_z = jnp.dot(
            jnp.concatenate([high, low, high], axis=1), fz_all[...], preferred_element_type=jnp.float32
        )
        tops, lows = [], []
        for k in range(3):
            g = along_z[k * grid_side : (k + 1) * grid_side, :128]
            h = along_z[k * grid_side : (k + 1) * grid_side, 128:]
            tops.append(turn_cos * g + turn_sin * h)
            lows.append(turn_cos * h - turn_sin * g)
        stacked = jnp.concatenate(
            [jnp.concatenate(tops, axis=1), jnp.concatenate(lows, axis=1)], axis=0
        )
        result = from_left(fy[...], stacked)
        for k in range(3):
            sent[:, plane * 3 + k, :] = result[:, k * 128 : (k + 1) * 128]
    for k in range(planes * 3, rows_sent):
        sent[:, k, :] = jnp.zeros((peers, 128), jnp.float32)


def emit_modes(state, wave_x, table, sent):
    turned = [times_i(v) for v in state]
    top = state + [wave_x * turned[1], wave_x * turned[2]]
    low = turned + [-wave_x * state[1], -wave_x * state[2]]
    stacked = jnp.concatenate(
        [jnp.concatenate(top, axis=1), jnp.concatenate(low, axis=1)], axis=0
    )
    result = from_left(table, stacked)
    for plane in range(planes):
        for k in range(5):
            sent[:, plane * 5 + k, :] = result[
                plane * peers : (plane + 1) * peers, k * 128 : (k + 1) * 128
            ]
    sent[:, planes * 5, :] = jnp.zeros((peers, 128), jnp.float32)


def start_kernel(state, wx, ix, sent):
    emit_modes([state[k] for k in range(3)], wx[...], ix[...], sent)


def modes_kernel(arrived, state, extra, wx, ly, lz, damp, gain, fx, ix, following, sent):
    fields = []
    for k in range(3):
        fields.append(
            jnp.concatenate([arrived[:, plane * 3 + k, :] for plane in range(planes)], axis=0)
        )
    packed = jnp.concatenate(fields, axis=1)
    turned = jnp.concatenate([-times_i(v) for v in fields], axis=1)
    spectrum = from_left(fx[...], jnp.concatenate([packed, turned], axis=0))
    n = [spectrum[:, k * 128 : (k + 1) * 128] for k in range(3)]
    wave_x, wave_y, wave_z = wx[...], ly[...], lz[...]
    divergence = (wave_x * n[0] + wave_y * n[1] + wave_z * n[2]) * gain[...]
    waves = [wave_x, wave_y, wave_z]
    fresh = []
    for k in range(3):
        moved = state[k] + time_step * (n[k] - waves[k] * divergence)
        fresh.append(damp[...] * moved + extra[k])
        following[k] = fresh[k]
    emit_modes(fresh, wave_x, ix[...], sent)


def chain_steps(place):
    tables = chain_tables()
    x, y, core = place
    wave_y = x * 16 + y * 4 + core
    wave_y = jnp.where(wave_y < M // 2, wave_y, wave_y - M)
    lane = jnp.arange(128, dtype=jnp.int32)
    lanes_y = (wave_y + lane // 64 * 2).astype(jnp.float32)[None, :]
    lanes_z = (lane % (M // 2)).astype(jnp.float32)[None, :]
    wave_x = jnp.asarray(tables["wave_x"])
    squared = wave_x * wave_x + lanes_y * lanes_y + lanes_z * lanes_z
    damp = jnp.exp(-viscosity * time_step * squared)
    gain = 1.0 / jnp.maximum(squared, 1.0)
    parcel = jax.ShapeDtypeStruct((peers, rows_sent, 128), jnp.float32)
    shape = jax.ShapeDtypeStruct((3, M, 128), jnp.float32)
    grid_step = pl.pallas_call(grid_kernel, out_shape=parcel, name="grid_step")
    modes_step = pl.pallas_call(modes_kernel, out_shape=(shape, parcel), name="modes_step")
    start_step = pl.pallas_call(start_kernel, out_shape=parcel, name="start_step")
    move = partial(lax.all_to_all, axis_name=ring, split_axis=0, concat_axis=0, tiled=True)
    grid_tables = [
        tables["inverse_y"],
        tables["turn_cos"],
        tables["turn_sin"],
        tables["iz_both"],
        tables["iz_high"],
        tables["fz_all"],
        tables["forward_y"],
        tables["lanes_y"],
        tables["lanes_z"],
    ]
    mode_tables = [
        wave_x, lanes_y, lanes_z, damp, gain, tables["forward_x"], tables["inverse_x"]
    ]

    def start(state):
        return start_step(state, wave_x, tables["inverse_x"])

    def grid_work(arrived):
        return grid_step(arrived, *grid_tables)

    def mode_work(arrived, state, extra):
        return modes_step(arrived, state, extra, *mode_tables)

    def follow(state, parcels, extra):
        return mode_work(move(grid_work(move(parcels))), state, extra)

    return start, follow, move, grid_work, mode_work


def chain_sweep(first, extras, place):
    start, follow = chain_steps(place)[:2]

    def turn(index, carried):
        state, parcels, history = carried
        extra = lax.dynamic_index_in_dim(extras, index, 0, keepdims=False)
        state, parcels = follow(state, parcels, extra)
        history = lax.dynamic_update_index_in_dim(history, state, index + 1, 0)
        return state, parcels, history

    history = jnp.zeros((16, 3, M, 128), jnp.float32)
    history = lax.dynamic_update_index_in_dim(history, first, 1, 0)
    return lax.fori_loop(1, 15, turn, (first, start(first), history))[2]


def to_ring(block, zh):
    pieces = jnp.moveaxis(block, 2, 0).reshape(4, 1, 3 * M // 2, 128)
    pieces = jnp.broadcast_to(pieces, (4, 2, 3 * M // 2, 128)).reshape(8, 3 * M // 2, 128)
    pieces = lax.all_to_all(pieces, ("x", "zh"), split_axis=0, concat_axis=0, tiled=True)
    pieces = lax.dynamic_slice_in_dim(pieces, zh * 4, 4, axis=0).reshape(2, 2, 3, M, M)
    return jnp.transpose(pieces, (0, 2, 3, 1, 4)).reshape(2, 3, M, 128)


def spread_payload(payload):
    copies = jnp.broadcast_to(payload.reshape(1, 6 * M, 128), (8, 6 * M, 128))
    gathered = lax.all_to_all(copies, ("zl", "zh"), split_axis=0, concat_axis=0, tiled=True)
    gathered = gathered.reshape(4, 2, 2, 3, M, 128)
    return jnp.transpose(gathered, (1, 2, 0, 3, 4, 5)).reshape(16, 3, M, 128)


def collect_slices(history, zl, zh):
    mine = lax.dynamic_index_in_dim(history.reshape(4, 4, 3, M, 2, M), zl, 1, keepdims=False)
    mine = lax.dynamic_index_in_dim(mine, zh, 3, keepdims=False)
    pieces = lax.all_to_all(
        mine.reshape(4, 3 * M // 2, 128), "x", split_axis=0, concat_axis=0, tiled=True
    )
    return jnp.moveaxis(pieces.reshape(4, 3, M, M), 0, 2)


def shards(start_states):
    x, zl, y, zh, core = [lax.axis_index(name) for name in ("x", "zl", "y", "zh", "core")]
    groups = 16
    member = (y * 2 + zh) * 2 + core
    layout = (4, 4, groups, member)
    place = (x, y, core)
    position = x * 4 + zl
    retained = start_states.shape[-1]
    stored = start_states.reshape(3, retained, start_states.shape[3], retained)
    spectral_state = project(stored, wave_grid(retained, layout))
    low_states = to_ring(restrict(spectral_state, M, groups), zh)
    fine_end, coarse_next = advance_both(spectral_state, low_states, place, layout)
    fine_low = restrict(fine_end, M, groups)
    low_ring = to_ring(fine_low, zh)
    opening = (zl == 0) & (zh == 0) & (jnp.arange(2) == 0)
    payload = jnp.where(opening[:, None, None, None], low_ring, low_ring - coarse_next)
    everything = spread_payload(payload)
    upper_band = jnp.where(shared_modes(retained, groups), 0.0, fine_end)
    previous = shifted(upper_band, ("x", "zl"), 1)
    history = chain_sweep(everything[0], everything, place)
    current = collect_slices(history, zl, zh)
    updated = prolong(current, retained, groups) + previous
    result = jnp.where(position == 0, spectral_state, updated)
    return result.reshape(1, result.shape[0], retained, result.shape[2], 1, retained)


def solution(mesh):
    split = Mesh(mesh.devices.reshape(4, 4, 4, 2, 2), ("x", "zl", "y", "zh", "core"))
    spec = P(("x", "zl"), None, None, None, ("y", "zh", "core"), None)
    return jax.shard_map(shards, mesh=split, in_specs=(spec,), out_specs=spec, check_vma=False)
```

```python
from functools import partial
import math

import jax
import jax.numpy as jnp
import numpy as np
from jax import lax
from jax.experimental import pallas as pl
from jax.experimental.pallas import tpu as pltpu
from jax.sharding import Mesh
from jax.sharding import PartitionSpec as P


M = 64


viscosity = 0.03
time_step = 0.004
highest = lax.Precision.HIGH


def shifted(block, axis, distance):
    devices = range(lax.axis_size(axis))
    route = [(i - distance, i) for i in devices if i - distance in devices]
    return lax.ppermute(block, axis, route)


def signed_wave(places, length):
    return jnp.where(places < length // 2, places, places - length)


def rotate(values):
    halfway = values.shape[-1] // 2
    return jnp.concatenate([-values[..., halfway:], values[..., :halfway]], axis=-1)


def trig_pair(outer, inner, extent, factor):
    residue = jnp.mod(outer[:, None] * inner[None, :], extent)
    radians = residue.astype(jnp.float32) * (2.0 * math.pi / extent)
    return (jnp.cos(radians) * factor, jnp.sin(radians) * factor)


def complex_apply(cosine_part, sine_part, values, contracted, direction_sign):
    kernel = jnp.stack(
        [
            jnp.stack([cosine_part, -direction_sign * sine_part]),
            jnp.stack([direction_sign * sine_part, cosine_part]),
        ]
    )
    halfway = values.shape[-1] // 2
    split = values.reshape(values.shape[:-1] + (2, halfway))
    if contracted == 1:
        pattern = "pqok,fkaqh->foaph"
    else:
        pattern = "pqok,flkqh->floph"
    result = jnp.einsum(pattern, kernel, split, precision=highest)
    return result.reshape(result.shape[:-2] + (2 * halfway,))


def inverse_z(extent, retained):
    halfway = retained // 2
    columns = jnp.arange(retained, dtype=jnp.int32)
    harmonic = columns % halfway
    weight = jnp.where(harmonic == 0, 1.0, 2.0) * retained ** (-0.5)
    residue = jnp.mod(harmonic[:, None] * jnp.arange(extent, dtype=jnp.int32)[None, :], extent)
    radians = residue.astype(jnp.float32) * (2.0 * math.pi / extent)
    return (
        jnp.where((columns < halfway)[:, None], jnp.cos(radians), -jnp.sin(radians))
        * weight[:, None]
    )


def forward_z(extent, retained):
    halfway = retained // 2
    columns = jnp.arange(retained, dtype=jnp.int32)
    harmonic = columns % halfway
    residue = jnp.mod(jnp.arange(extent, dtype=jnp.int32)[:, None] * harmonic[None, :], extent)
    radians = residue.astype(jnp.float32) * (2.0 * math.pi / extent)
    return jnp.where((columns < halfway)[None, :], jnp.cos(radians), -jnp.sin(radians)) * (
        math.sqrt(retained) / extent
    )


def exchange(block, split_dim, concat_dim):
    return lax.all_to_all(
        block, ("y", "zh", "core"), split_axis=split_dim, concat_axis=concat_dim, tiled=True
    )


def wave_y_places(retained, groups):
    local_rows = retained // groups
    places = jnp.arange(retained, dtype=jnp.int32)
    return signed_wave(places % local_rows * groups + places // local_rows, retained)


def inverse_tail(portion, extent, groups):
    retained = portion.shape[2]
    points = jnp.arange(extent, dtype=jnp.int32)
    wave_y = wave_y_places(retained, groups)
    cosine_part, sine_part = trig_pair(points, wave_y, extent, retained ** (-0.5))
    along_y = complex_apply(cosine_part, sine_part, portion, 2, 1.0)
    return jnp.einsum("flyr,rz->flyz", along_y, inverse_z(extent, retained), precision=highest)


def forward_tail(portion, retained):
    extent = portion.shape[1]
    points = jnp.arange(extent, dtype=jnp.int32)
    wave_x = signed_wave(jnp.arange(retained, dtype=jnp.int32), retained)
    cosine_part, sine_part = trig_pair(wave_x, points, extent, math.sqrt(retained) / extent)
    return complex_apply(cosine_part, sine_part, portion, 1, -1.0)


def spread_x(coeffs, wavegrid, extent):
    wave_x = wavegrid[0]
    retained = coeffs.shape[1]
    points = jnp.arange(extent, dtype=jnp.int32)
    wave_rows = signed_wave(jnp.arange(retained, dtype=jnp.int32), retained)
    cosine_part, sine_part = trig_pair(points, wave_rows, extent, retained ** (-0.5))
    moved = complex_apply(cosine_part, sine_part, coeffs, 1, 1.0)
    slopes = complex_apply(cosine_part, sine_part, wave_x * coeffs[1:3], 1, 1.0)
    return moved, slopes


def to_physical(moved, slopes, wavegrid, extent, groups):
    wave_z = wavegrid[2]
    retained = moved.shape[2]
    all_y = wave_y_places(retained, groups).astype(jnp.float32)[None, :, None]
    velocity = inverse_tail(moved, extent, groups)
    curl_x = rotate(all_y * moved[2] - wave_z * moved[1])
    curl_y = rotate(wave_z * moved[0] - slopes[1])
    curl_z = rotate(slopes[0] - all_y * moved[0])
    return velocity, inverse_tail(jnp.stack([curl_x, curl_y, curl_z]), extent, groups)


def along_planes(fields, retained, groups):
    extent = fields.shape[-1]
    along_z = jnp.einsum("flyz,zr->flyr", fields, forward_z(extent, retained), precision=highest)
    wave_y = wave_y_places(retained, groups)
    cosine_part, sine_part = trig_pair(
        wave_y, jnp.arange(extent, dtype=jnp.int32), extent, math.sqrt(retained) / extent
    )
    return complex_apply(cosine_part, sine_part, along_z, 2, -1.0)


def wave_grid(retained, layout):
    _, _, groups, member = layout
    places = jnp.arange(retained, dtype=jnp.int32)
    wave_x = signed_wave(places, retained).astype(jnp.float32)[:, None, None]
    local_places = jnp.arange(retained // groups, dtype=jnp.int32)
    wave_y = signed_wave(local_places * groups + member, retained).astype(jnp.float32)[
        None, :, None
    ]
    wave_z = (places % (retained // 2)).astype(jnp.float32)[None, None, :]
    return (wave_x, wave_y, wave_z)


def project(coeffs, wavegrid):
    wave_x, wave_y, wave_z = wavegrid
    squared = wave_x * wave_x + wave_y * wave_y + wave_z * wave_z
    divergence = (wave_x * coeffs[0] + wave_y * coeffs[1] + wave_z * coeffs[2]) / jnp.maximum(
        squared, 1.0
    )
    return jnp.stack(
        [
            coeffs[0] - wave_x * divergence,
            coeffs[1] - wave_y * divergence,
            coeffs[2] - wave_z * divergence,
        ]
    )


def cross_parts(first_field, second_field):
    return [
        first_field[1] * second_field[2] - first_field[2] * second_field[1],
        first_field[2] * second_field[0] - first_field[0] * second_field[2],
        first_field[0] * second_field[1] - first_field[1] * second_field[0],
    ]


def advance_both(coeffs, low_states, place, layout):
    groups = layout[2]
    retained = coeffs.shape[1]
    extent = 3 * retained // 2
    wavegrid = wave_grid(retained, layout)
    start, _, move, grid_work, mode_work = chain_steps(place)
    moved, slopes = spread_x(coeffs, wavegrid, extent)
    moved, slopes, low_states = lax.optimization_barrier((moved, slopes, low_states))
    moved = exchange(moved, 1, 2)
    moved, slopes = lax.optimization_barrier((moved, slopes))
    slopes = exchange(slopes, 1, 2)
    parcels = jnp.concatenate([start(low_states[0]), start(low_states[1])], axis=1)
    slopes, parcels = lax.optimization_barrier((slopes, parcels))
    arrived = move(parcels)
    velocity, curl = to_physical(moved, slopes, wavegrid, extent, groups)
    velocity, curl, arrived = lax.optimization_barrier((velocity, curl, arrived))
    products = [grid_work(arrived[:, :rows_sent]), grid_work(arrived[:, rows_sent:])]
    products = jnp.concatenate(products, axis=1)
    parts = [
        exchange(along_planes(part[None], retained, groups), 2, 1)
        for part in cross_parts(velocity, curl)
    ]
    parts, products = lax.optimization_barrier((parts, products))
    arrived = move(products)
    nonlinear = jnp.concatenate([forward_tail(part, retained) for part in parts])
    wave_x, wave_y, wave_z = wavegrid
    squared = wave_x * wave_x + wave_y * wave_y + wave_z * wave_z
    damping = jnp.exp(-viscosity * time_step * squared)
    fine_end = damping * (coeffs + time_step * project(nonlinear, wavegrid))
    fine_end, arrived = lax.optimization_barrier((fine_end, arrived))
    nothing = jnp.zeros((3, M, 128), jnp.float32)
    first = mode_work(arrived[:, :rows_sent], low_states[0], nothing)[0]
    second = mode_work(arrived[:, rows_sent:], low_states[1], nothing)[0]
    return fine_end, jnp.stack([first, second])


def restrict(coeffs, kept, groups):
    halfway = kept // 2
    retained = coeffs.shape[1]
    rows_kept = jnp.concatenate([coeffs[:, :halfway], coeffs[:, retained - halfway :]], axis=1)
    local_rows = coeffs.shape[2]
    local_kept = kept // groups // 2
    rows_kept = jnp.concatenate(
        [rows_kept[:, :, :local_kept], rows_kept[:, :, local_rows - local_kept :]], axis=2
    )
    columns_half = coeffs.shape[3] // 2
    return jnp.concatenate(
        [rows_kept[..., :halfway], rows_kept[..., columns_half : columns_half + halfway]], axis=3
    )


def shared_modes(retained, groups):
    limit = M // 2
    local_rows = retained // groups
    local_limit = limit // groups
    along_x = jnp.arange(retained, dtype=jnp.int32)
    along_y = jnp.arange(local_rows, dtype=jnp.int32)
    along_z = jnp.arange(retained, dtype=jnp.int32) % (retained // 2)
    keep_x = (along_x < limit) | (along_x >= retained - limit)
    keep_y = (along_y < local_limit) | (along_y >= local_rows - local_limit)
    keep_z = along_z < limit
    return keep_x[:, None, None] & keep_y[None, :, None] & keep_z[None, None, :]


def prolong(coeffs, retained, groups):
    components, kept, local_kept, width = coeffs.shape
    halfway = kept // 2
    zeros_x = jnp.zeros((components, retained - kept, local_kept, width), jnp.float32)
    wider = jnp.concatenate([coeffs[:, :halfway], zeros_x, coeffs[:, halfway:]], axis=1)
    local_rows = retained // groups
    split_rows = local_kept // 2
    zeros_y = jnp.zeros((components, retained, local_rows - local_kept, width), jnp.float32)
    wider = jnp.concatenate([wider[:, :, :split_rows], zeros_y, wider[:, :, split_rows:]], axis=2)
    zeros_z = jnp.zeros((components, retained, local_rows, retained // 2 - halfway), jnp.float32)
    return jnp.concatenate([wider[..., :halfway], zeros_z, wider[..., halfway:], zeros_z], axis=3)


ring = ("x", "y", "core")
peers = 32
planes = 3
rows_sent = 16
grid_side = 3 * M // 2


def two_parts(values):
    high = values.astype(jnp.bfloat16)
    return high, (values - high.astype(jnp.float32)).astype(jnp.bfloat16)


def table_parts(table):
    table = table.astype(np.float32)
    high = table.astype(jnp.bfloat16)
    low = (table - high.astype(np.float32)).astype(jnp.bfloat16)
    return high, low


def left_table(table):
    high, low = table_parts(table)
    return np.concatenate([high, high, low], axis=1)


def from_left(table, values):
    high, low = two_parts(values)
    stacked = jnp.concatenate([high, low, high], axis=0)
    return jnp.dot(table, stacked, preferred_element_type=jnp.float32)


def chain_tables():
    points = np.arange(grid_side)
    step = 2.0 * np.pi / grid_side
    member = np.arange(peers)
    wave_y = member // 8 * 16 + member // 2 % 4 * 4 + member % 2
    wave_y = np.where(wave_y < M // 2, wave_y, wave_y - M)
    angle_y = np.outer(points, wave_y) * step
    lanes = np.arange(128)
    pair = lanes // 64
    half = M // 2
    wave_z = lanes % half
    imaginary = lanes % 64 >= half
    inverse_y = np.concatenate([np.cos(angle_y), np.sin(angle_y)], axis=0) * M**-0.5
    twist = np.outer(points, 2 * pair) * step
    turn_cos, turn_sin = np.cos(twist), np.sin(twist)
    angle_z = np.outer(wave_z, points) * step
    weight = (np.where(wave_z == 0, 1.0, 2.0) * M**-0.5)[:, None]
    plain = np.where(imaginary[:, None], -np.sin(angle_z), np.cos(angle_z)) * weight
    turned = np.where(imaginary[:, None], -np.cos(angle_z), -np.sin(angle_z)) * weight
    inverse_z = np.zeros((256, 128))
    inverse_z[:128, :grid_side] = plain
    inverse_z[128:, :grid_side] = turned
    iz_high, iz_low = table_parts(inverse_z)
    iz_both = np.concatenate([iz_high, iz_low], axis=1)
    scale = M**0.5 / grid_side
    forward_z = np.zeros((128, 256))
    forward_z[:grid_side, :128] = np.where(imaginary[:, None], -np.sin(angle_z), np.cos(angle_z)).T * scale
    forward_z[:grid_side, 128:] = np.where(imaginary[:, None], -np.cos(angle_z), -np.sin(angle_z)).T * scale
    fz_high, fz_low = table_parts(forward_z)
    fz_all = np.concatenate([fz_high, fz_high, fz_low], axis=0)
    forward_y = np.concatenate([np.cos(angle_y.T), np.sin(angle_y.T)], axis=1) * scale
    member_x = np.arange(grid_side)
    wave_x = np.where(np.arange(M) < half, np.arange(M), np.arange(M) - M)
    angle_x = np.outer(wave_x, member_x) * step
    forward_x = np.concatenate([np.cos(angle_x), np.sin(angle_x)], axis=1) * scale
    inverse_x = np.concatenate([np.cos(angle_x.T), np.sin(angle_x.T)], axis=1) * M**-0.5
    lanes_y = np.broadcast_to(wave_y[:, None] + 2 * pair[None, :], (peers, 128))
    lanes_z = np.broadcast_to(wave_z[None, :], (peers, 128))
    return {
        "inverse_y": left_table(inverse_y),
        "turn_cos": turn_cos.astype(np.float32),
        "turn_sin": turn_sin.astype(np.float32),
        "iz_both": iz_both,
        "iz_high": iz_high,
        "fz_all": fz_all,
        "forward_y": left_table(forward_y),
        "forward_x": left_table(forward_x),
        "inverse_x": left_table(inverse_x),
        "lanes_y": lanes_y.astype(np.float32),
        "lanes_z": lanes_z.astype(np.float32),
        "wave_x": np.broadcast_to(wave_x[:, None], (M, 128)).astype(np.float32),
    }


def times_i(values):
    lane = lax.broadcasted_iota(jnp.int32, values.shape, 1)
    ahead = pltpu.roll(values, 96, 1)
    behind = pltpu.roll(values, 32, 1)
    return jnp.where(lane % 64 < 32, -ahead, behind)


def grid_kernel(arrived, iy, tc, ts, iz_both, iz_high, fz_all, fy, ly, lz, sent):
    wave_y, wave_z = ly[...], lz[...]
    turn_cos, turn_sin = tc[...], ts[...]
    for plane in range(planes):
        ux, uy, uz, dy, dz = [arrived[:, plane * 5 + k, :] for k in range(5)]
        wx = times_i(wave_y * uz - wave_z * uy)
        wy = times_i(wave_z * ux) - dz
        wz = dy - times_i(wave_y * ux)
        packed = jnp.concatenate([ux, uy, uz, wx, wy, wz], axis=1)
        along_y = from_left(iy[...], packed)
        pieces = []
        for k in range(6):
            c = along_y[:grid_side, k * 128 : (k + 1) * 128]
            s = along_y[grid_side:, k * 128 : (k + 1) * 128]
            pieces.append(
                jnp.concatenate([turn_cos * c - turn_sin * s, turn_cos * s + turn_sin * c], axis=1)
            )
        high, low = two_parts(jnp.concatenate(pieces, axis=0))
        wide = jnp.dot(high, iz_both[...], preferred_element_type=jnp.float32)
        rest = jnp.dot(low, iz_high[...], preferred_element_type=jnp.float32)
        field = wide[:, :128] + wide[:, 128:] + rest
        f = [field[k * grid_side : (k + 1) * grid_side] for k in range(6)]
        product = jnp.concatenate(
            [
                f[1] * f[5] - f[2] * f[4],
                f[2] * f[3] - f[0] * f[5],
                f[0] * f[4] - f[1] * f[3],
            ],
            axis=0,
        )
        high, low = two_parts(product)
        along_z = jnp.dot(
            jnp.concatenate([high, low, high], axis=1), fz_all[...], preferred_element_type=jnp.float32
        )
        tops, lows = [], []
        for k in range(3):
            g = along_z[k * grid_side : (k + 1) * grid_side, :128]
            h = along_z[k * grid_side : (k + 1) * grid_side, 128:]
            tops.append(turn_cos * g + turn_sin * h)
            lows.append(turn_cos * h - turn_sin * g)
        stacked = jnp.concatenate(
            [jnp.concatenate(tops, axis=1), jnp.concatenate(lows, axis=1)], axis=0
        )
        result = from_left(fy[...], stacked)
        for k in range(3):
            sent[:, plane * 3 + k, :] = result[:, k * 128 : (k + 1) * 128]
    for k in range(planes * 3, rows_sent):
        sent[:, k, :] = jnp.zeros((peers, 128), jnp.float32)


def emit_modes(state, wave_x, table, sent):
    turned = [times_i(v) for v in state]
    top = state + [wave_x * turned[1], wave_x * turned[2]]
    low = turned + [-wave_x * state[1], -wave_x * state[2]]
    stacked = jnp.concatenate(
        [jnp.concatenate(top, axis=1), jnp.concatenate(low, axis=1)], axis=0
    )
    result = from_left(table, stacked)
    for plane in range(planes):
        for k in range(5):
            sent[:, plane * 5 + k, :] = result[
                plane * peers : (plane + 1) * peers, k * 128 : (k + 1) * 128
            ]
    sent[:, planes * 5, :] = jnp.zeros((peers, 128), jnp.float32)


def start_kernel(state, wx, ix, sent):
    emit_modes([state[k] for k in range(3)], wx[...], ix[...], sent)


def modes_kernel(arrived, state, extra, wx, ly, lz, damp, gain, fx, ix, following, sent):
    fields = []
    for k in range(3):
        fields.append(
            jnp.concatenate([arrived[:, plane * 3 + k, :] for plane in range(planes)], axis=0)
        )
    packed = jnp.concatenate(fields, axis=1)
    turned = jnp.concatenate([-times_i(v) for v in fields], axis=1)
    spectrum = from_left(fx[...], jnp.concatenate([packed, turned], axis=0))
    n = [spectrum[:, k * 128 : (k + 1) * 128] for k in range(3)]
    wave_x, wave_y, wave_z = wx[...], ly[...], lz[...]
    divergence = (wave_x * n[0] + wave_y * n[1] + wave_z * n[2]) * gain[...]
    waves = [wave_x, wave_y, wave_z]
    fresh = []
    for k in range(3):
        moved = state[k] + time_step * (n[k] - waves[k] * divergence)
        fresh.append(damp[...] * moved + extra[k])
        following[k] = fresh[k]
    emit_modes(fresh, wave_x, ix[...], sent)


def near(values):
    return pltpu.with_memory_space_constraint(values, pltpu.VMEM)


def chain_steps(place):
    tables = chain_tables()
    x, y, core = place
    wave_y = x * 16 + y * 4 + core
    wave_y = jnp.where(wave_y < M // 2, wave_y, wave_y - M)
    lane = jnp.arange(128, dtype=jnp.int32)
    lanes_y = (wave_y + lane // 64 * 2).astype(jnp.float32)[None, :]
    lanes_z = (lane % (M // 2)).astype(jnp.float32)[None, :]
    wave_x = jnp.asarray(tables["wave_x"])
    squared = wave_x * wave_x + lanes_y * lanes_y + lanes_z * lanes_z
    damp = jnp.exp(-viscosity * time_step * squared)
    gain = 1.0 / jnp.maximum(squared, 1.0)
    parcel = pltpu.VMEM((peers, rows_sent, 128), jnp.float32)
    shape = jax.ShapeDtypeStruct((3, M, 128), jnp.float32)
    grid_step = pl.pallas_call(grid_kernel, out_shape=parcel, name="grid_step")
    modes_step = pl.pallas_call(modes_kernel, out_shape=(shape, parcel), name="modes_step")
    start_step = pl.pallas_call(start_kernel, out_shape=parcel, name="start_step")
    move = partial(lax.all_to_all, axis_name=ring, split_axis=0, concat_axis=0, tiled=True)
    grid_tables = [
        tables["inverse_y"],
        tables["turn_cos"],
        tables["turn_sin"],
        tables["iz_both"],
        tables["iz_high"],
        tables["fz_all"],
        tables["forward_y"],
        tables["lanes_y"],
        tables["lanes_z"],
    ]
    mode_tables = [
        wave_x, lanes_y, lanes_z, damp, gain, tables["forward_x"], tables["inverse_x"]
    ]

    def start(state):
        return start_step(state, wave_x, tables["inverse_x"])

    def grid_work(arrived):
        return grid_step(near(arrived), *grid_tables)

    def mode_work(arrived, state, extra):
        return modes_step(near(arrived), state, extra, *mode_tables)

    def follow(state, parcels, extra):
        return mode_work(move(grid_work(move(parcels))), state, extra)

    return start, follow, move, grid_work, mode_work


def chain_sweep(first, extras, place):
    start, follow = chain_steps(place)[:2]

    def turn(index, carried):
        state, parcels, history = carried
        extra = lax.dynamic_index_in_dim(extras, index, 0, keepdims=False)
        state, parcels = follow(state, parcels, extra)
        history = lax.dynamic_update_index_in_dim(history, state, index + 1, 0)
        return state, parcels, history

    history = jnp.zeros((16, 3, M, 128), jnp.float32)
    history = lax.dynamic_update_index_in_dim(history, first, 1, 0)
    return lax.fori_loop(1, 15, turn, (first, start(first), history))[2]


def to_ring(block, zh):
    pieces = jnp.moveaxis(block, 2, 0).reshape(4, 1, 3 * M // 2, 128)
    pieces = jnp.broadcast_to(pieces, (4, 2, 3 * M // 2, 128)).reshape(8, 3 * M // 2, 128)
    pieces = lax.all_to_all(pieces, ("x", "zh"), split_axis=0, concat_axis=0, tiled=True)
    pieces = lax.dynamic_slice_in_dim(pieces, zh * 4, 4, axis=0).reshape(2, 2, 3, M, M)
    return jnp.transpose(pieces, (0, 2, 3, 1, 4)).reshape(2, 3, M, 128)


def spread_payload(payload):
    copies = jnp.broadcast_to(payload.reshape(1, 6 * M, 128), (8, 6 * M, 128))
    gathered = lax.all_to_all(copies, ("zl", "zh"), split_axis=0, concat_axis=0, tiled=True)
    gathered = gathered.reshape(4, 2, 2, 3, M, 128)
    return jnp.transpose(gathered, (1, 2, 0, 3, 4, 5)).reshape(16, 3, M, 128)


def collect_slices(history, zl, zh):
    mine = lax.dynamic_index_in_dim(history.reshape(4, 4, 3, M, 2, M), zl, 1, keepdims=False)
    mine = lax.dynamic_index_in_dim(mine, zh, 3, keepdims=False)
    pieces = lax.all_to_all(
        mine.reshape(4, 3 * M // 2, 128), "x", split_axis=0, concat_axis=0, tiled=True
    )
    return jnp.moveaxis(pieces.reshape(4, 3, M, M), 0, 2)


def shards(start_states):
    x, zl, y, zh, core = [lax.axis_index(name) for name in ("x", "zl", "y", "zh", "core")]
    groups = 16
    member = (y * 2 + zh) * 2 + core
    layout = (4, 4, groups, member)
    place = (x, y, core)
    position = x * 4 + zl
    retained = start_states.shape[-1]
    stored = start_states.reshape(3, retained, start_states.shape[3], retained)
    spectral_state = project(stored, wave_grid(retained, layout))
    low_states = to_ring(restrict(spectral_state, M, groups), zh)
    fine_end, coarse_next = advance_both(spectral_state, low_states, place, layout)
    fine_low = restrict(fine_end, M, groups)
    low_ring = to_ring(fine_low, zh)
    opening = (zl == 0) & (zh == 0) & (jnp.arange(2) == 0)
    payload = jnp.where(opening[:, None, None, None], low_ring, low_ring - coarse_next)
    everything = spread_payload(payload)
    upper_band = jnp.where(shared_modes(retained, groups), 0.0, fine_end)
    previous = shifted(upper_band, ("x", "zl"), 1)
    history = chain_sweep(everything[0], everything, place)
    current = collect_slices(history, zl, zh)
    updated = prolong(current, retained, groups) + previous
    result = jnp.where(position == 0, spectral_state, updated)
    return result.reshape(1, result.shape[0], retained, result.shape[2], 1, retained)


def solution(mesh):
    split = Mesh(mesh.devices.reshape(4, 4, 4, 2, 2), ("x", "zl", "y", "zh", "core"))
    spec = P(("x", "zl"), None, None, None, ("y", "zh", "core"), None)
    return jax.shard_map(shards, mesh=split, in_specs=(spec,), out_specs=spec, check_vma=False)
```

```python
from functools import partial
import math

import jax
import jax.numpy as jnp
import numpy as np
from jax import lax
from jax.experimental import pallas as pl
from jax.experimental.pallas import tpu as pltpu
from jax.sharding import Mesh
from jax.sharding import PartitionSpec as P


M = 64


viscosity = 0.03
time_step = 0.004
highest = lax.Precision.HIGH


def shifted(block, axis, distance):
    devices = range(lax.axis_size(axis))
    route = [(i - distance, i) for i in devices if i - distance in devices]
    return lax.ppermute(block, axis, route)


def signed_wave(places, length):
    return jnp.where(places < length // 2, places, places - length)


def rotate(values):
    halfway = values.shape[-1] // 2
    return jnp.concatenate([-values[..., halfway:], values[..., :halfway]], axis=-1)


def trig_pair(outer, inner, extent, factor):
    residue = jnp.mod(outer[:, None] * inner[None, :], extent)
    radians = residue.astype(jnp.float32) * (2.0 * math.pi / extent)
    return (jnp.cos(radians) * factor, jnp.sin(radians) * factor)


def complex_apply(cosine_part, sine_part, values, contracted, direction_sign):
    kernel = jnp.stack(
        [
            jnp.stack([cosine_part, -direction_sign * sine_part]),
            jnp.stack([direction_sign * sine_part, cosine_part]),
        ]
    )
    halfway = values.shape[-1] // 2
    split = values.reshape(values.shape[:-1] + (2, halfway))
    if contracted == 1:
        pattern = "pqok,fkaqh->foaph"
    else:
        pattern = "pqok,flkqh->floph"
    result = jnp.einsum(pattern, kernel, split, precision=highest)
    return result.reshape(result.shape[:-2] + (2 * halfway,))


def inverse_z(extent, retained):
    halfway = retained // 2
    columns = jnp.arange(retained, dtype=jnp.int32)
    harmonic = columns % halfway
    weight = jnp.where(harmonic == 0, 1.0, 2.0) * retained ** (-0.5)
    residue = jnp.mod(harmonic[:, None] * jnp.arange(extent, dtype=jnp.int32)[None, :], extent)
    radians = residue.astype(jnp.float32) * (2.0 * math.pi / extent)
    return (
        jnp.where((columns < halfway)[:, None], jnp.cos(radians), -jnp.sin(radians))
        * weight[:, None]
    )


def forward_z(extent, retained):
    halfway = retained // 2
    columns = jnp.arange(retained, dtype=jnp.int32)
    harmonic = columns % halfway
    residue = jnp.mod(jnp.arange(extent, dtype=jnp.int32)[:, None] * harmonic[None, :], extent)
    radians = residue.astype(jnp.float32) * (2.0 * math.pi / extent)
    return jnp.where((columns < halfway)[None, :], jnp.cos(radians), -jnp.sin(radians)) * (
        math.sqrt(retained) / extent
    )


def exchange(block, split_dim, concat_dim):
    return lax.all_to_all(
        block, ("y", "zh", "core"), split_axis=split_dim, concat_axis=concat_dim, tiled=True
    )


def wave_y_places(retained, groups):
    local_rows = retained // groups
    places = jnp.arange(retained, dtype=jnp.int32)
    return signed_wave(places % local_rows * groups + places // local_rows, retained)


def inverse_tail(portion, extent, groups):
    retained = portion.shape[2]
    points = jnp.arange(extent, dtype=jnp.int32)
    wave_y = wave_y_places(retained, groups)
    cosine_part, sine_part = trig_pair(points, wave_y, extent, retained ** (-0.5))
    along_y = complex_apply(cosine_part, sine_part, portion, 2, 1.0)
    return jnp.einsum("flyr,rz->flyz", along_y, inverse_z(extent, retained), precision=highest)


def forward_tail(portion, retained):
    extent = portion.shape[1]
    points = jnp.arange(extent, dtype=jnp.int32)
    wave_x = signed_wave(jnp.arange(retained, dtype=jnp.int32), retained)
    cosine_part, sine_part = trig_pair(wave_x, points, extent, math.sqrt(retained) / extent)
    return complex_apply(cosine_part, sine_part, portion, 1, -1.0)


def spread_x(coeffs, wavegrid, extent):
    wave_x = wavegrid[0]
    retained = coeffs.shape[1]
    points = jnp.arange(extent, dtype=jnp.int32)
    wave_rows = signed_wave(jnp.arange(retained, dtype=jnp.int32), retained)
    cosine_part, sine_part = trig_pair(points, wave_rows, extent, retained ** (-0.5))
    moved = complex_apply(cosine_part, sine_part, coeffs, 1, 1.0)
    slopes = complex_apply(cosine_part, sine_part, wave_x * coeffs[1:3], 1, 1.0)
    return moved, slopes


def to_physical(moved, slopes, wavegrid, extent, groups):
    wave_z = wavegrid[2]
    retained = moved.shape[2]
    all_y = wave_y_places(retained, groups).astype(jnp.float32)[None, :, None]
    velocity = inverse_tail(moved, extent, groups)
    curl_x = rotate(all_y * moved[2] - wave_z * moved[1])
    curl_y = rotate(wave_z * moved[0] - slopes[1])
    curl_z = rotate(slopes[0] - all_y * moved[0])
    return velocity, inverse_tail(jnp.stack([curl_x, curl_y, curl_z]), extent, groups)


def along_planes(fields, retained, groups):
    extent = fields.shape[-1]
    along_z = jnp.einsum("flyz,zr->flyr", fields, forward_z(extent, retained), precision=highest)
    wave_y = wave_y_places(retained, groups)
    cosine_part, sine_part = trig_pair(
        wave_y, jnp.arange(extent, dtype=jnp.int32), extent, math.sqrt(retained) / extent
    )
    return complex_apply(cosine_part, sine_part, along_z, 2, -1.0)


def wave_grid(retained, layout):
    _, _, groups, member = layout
    places = jnp.arange(retained, dtype=jnp.int32)
    wave_x = signed_wave(places, retained).astype(jnp.float32)[:, None, None]
    local_places = jnp.arange(retained // groups, dtype=jnp.int32)
    wave_y = signed_wave(local_places * groups + member, retained).astype(jnp.float32)[
        None, :, None
    ]
    wave_z = (places % (retained // 2)).astype(jnp.float32)[None, None, :]
    return (wave_x, wave_y, wave_z)


def project(coeffs, wavegrid):
    wave_x, wave_y, wave_z = wavegrid
    squared = wave_x * wave_x + wave_y * wave_y + wave_z * wave_z
    divergence = (wave_x * coeffs[0] + wave_y * coeffs[1] + wave_z * coeffs[2]) / jnp.maximum(
        squared, 1.0
    )
    return jnp.stack(
        [
            coeffs[0] - wave_x * divergence,
            coeffs[1] - wave_y * divergence,
            coeffs[2] - wave_z * divergence,
        ]
    )


def cross_parts(first_field, second_field):
    return [
        first_field[1] * second_field[2] - first_field[2] * second_field[1],
        first_field[2] * second_field[0] - first_field[0] * second_field[2],
        first_field[0] * second_field[1] - first_field[1] * second_field[0],
    ]


def advance_both(coeffs, low_states, place, layout):
    groups = layout[2]
    retained = coeffs.shape[1]
    extent = 3 * retained // 2
    wavegrid = wave_grid(retained, layout)
    start, _, move, grid_work, mode_work = chain_steps(place)
    moved, slopes = spread_x(coeffs, wavegrid, extent)
    moved, slopes, low_states = lax.optimization_barrier((moved, slopes, low_states))
    moved = exchange(moved, 1, 2)
    moved, slopes = lax.optimization_barrier((moved, slopes))
    slopes = exchange(slopes, 1, 2)
    parcels = jnp.concatenate([start(low_states[0]), start(low_states[1])], axis=2)
    slopes, parcels = lax.optimization_barrier((slopes, parcels))
    arrived = move(parcels)
    velocity, curl = to_physical(moved, slopes, wavegrid, extent, groups)
    velocity, curl, arrived = lax.optimization_barrier((velocity, curl, arrived))
    products = [grid_work(arrived[..., : planes * 640]), grid_work(arrived[..., planes * 640 :])]
    products = jnp.concatenate(products, axis=2)
    parts = [
        exchange(along_planes(part[None], retained, groups), 2, 1)
        for part in cross_parts(velocity, curl)
    ]
    parts, products = lax.optimization_barrier((parts, products))
    arrived = move(products)
    nonlinear = jnp.concatenate([forward_tail(part, retained) for part in parts])
    wave_x, wave_y, wave_z = wavegrid
    squared = wave_x * wave_x + wave_y * wave_y + wave_z * wave_z
    damping = jnp.exp(-viscosity * time_step * squared)
    fine_end = damping * (coeffs + time_step * project(nonlinear, wavegrid))
    fine_end, arrived = lax.optimization_barrier((fine_end, arrived))
    nothing = jnp.zeros((3, M, 128), jnp.float32)
    first = mode_work(arrived[..., : planes * 3 * 128], low_states[0], nothing)[0]
    second = mode_work(arrived[..., planes * 3 * 128 :], low_states[1], nothing)[0]
    return fine_end, jnp.stack([first, second])


def restrict(coeffs, kept, groups):
    halfway = kept // 2
    retained = coeffs.shape[1]
    rows_kept = jnp.concatenate([coeffs[:, :halfway], coeffs[:, retained - halfway :]], axis=1)
    local_rows = coeffs.shape[2]
    local_kept = kept // groups // 2
    rows_kept = jnp.concatenate(
        [rows_kept[:, :, :local_kept], rows_kept[:, :, local_rows - local_kept :]], axis=2
    )
    columns_half = coeffs.shape[3] // 2
    return jnp.concatenate(
        [rows_kept[..., :halfway], rows_kept[..., columns_half : columns_half + halfway]], axis=3
    )


def shared_modes(retained, groups):
    limit = M // 2
    local_rows = retained // groups
    local_limit = limit // groups
    along_x = jnp.arange(retained, dtype=jnp.int32)
    along_y = jnp.arange(local_rows, dtype=jnp.int32)
    along_z = jnp.arange(retained, dtype=jnp.int32) % (retained // 2)
    keep_x = (along_x < limit) | (along_x >= retained - limit)
    keep_y = (along_y < local_limit) | (along_y >= local_rows - local_limit)
    keep_z = along_z < limit
    return keep_x[:, None, None] & keep_y[None, :, None] & keep_z[None, None, :]


def prolong(coeffs, retained, groups):
    components, kept, local_kept, width = coeffs.shape
    halfway = kept // 2
    zeros_x = jnp.zeros((components, retained - kept, local_kept, width), jnp.float32)
    wider = jnp.concatenate([coeffs[:, :halfway], zeros_x, coeffs[:, halfway:]], axis=1)
    local_rows = retained // groups
    split_rows = local_kept // 2
    zeros_y = jnp.zeros((components, retained, local_rows - local_kept, width), jnp.float32)
    wider = jnp.concatenate([wider[:, :, :split_rows], zeros_y, wider[:, :, split_rows:]], axis=2)
    zeros_z = jnp.zeros((components, retained, local_rows, retained // 2 - halfway), jnp.float32)
    return jnp.concatenate([wider[..., :halfway], zeros_z, wider[..., halfway:], zeros_z], axis=3)


ring = ("x", "y", "core")
peers = 32
planes = 3
grid_side = 3 * M // 2


def two_parts(values):
    high = values.astype(jnp.bfloat16)
    return high, (values - high.astype(jnp.float32)).astype(jnp.bfloat16)


def table_parts(table):
    table = table.astype(np.float32)
    high = table.astype(jnp.bfloat16)
    low = (table - high.astype(np.float32)).astype(jnp.bfloat16)
    return high, low


def left_table(table):
    high, low = table_parts(table)
    return np.concatenate([high, high, low], axis=1)


def from_left(table, values):
    high, low = two_parts(values)
    stacked = jnp.concatenate([high, low, high], axis=0)
    return jnp.dot(table, stacked, preferred_element_type=jnp.float32)


def chain_tables():
    points = np.arange(grid_side)
    step = 2.0 * np.pi / grid_side
    member = np.arange(peers)
    wave_y = member // 8 * 16 + member // 2 % 4 * 4 + member % 2
    wave_y = np.where(wave_y < M // 2, wave_y, wave_y - M)
    angle_y = np.outer(points, wave_y) * step
    lanes = np.arange(128)
    pair = lanes // 64
    half = M // 2
    wave_z = lanes % half
    imaginary = lanes % 64 >= half
    inverse_y = np.concatenate([np.cos(angle_y), np.sin(angle_y)], axis=0) * M**-0.5
    twist = np.outer(points, 2 * pair) * step
    turn_cos, turn_sin = np.cos(twist), np.sin(twist)
    angle_z = np.outer(wave_z, points) * step
    weight = (np.where(wave_z == 0, 1.0, 2.0) * M**-0.5)[:, None]
    plain = np.where(imaginary[:, None], -np.sin(angle_z), np.cos(angle_z)) * weight
    turned = np.where(imaginary[:, None], -np.cos(angle_z), -np.sin(angle_z)) * weight
    inverse_z = np.zeros((256, 128))
    inverse_z[:128, :grid_side] = plain
    inverse_z[128:, :grid_side] = turned
    iz_high, iz_low = table_parts(inverse_z)
    iz_both = np.concatenate([iz_high, iz_low], axis=1)
    scale = M**0.5 / grid_side
    forward_z = np.zeros((128, 256))
    forward_z[:grid_side, :128] = np.where(imaginary[:, None], -np.sin(angle_z), np.cos(angle_z)).T * scale
    forward_z[:grid_side, 128:] = np.where(imaginary[:, None], -np.cos(angle_z), -np.sin(angle_z)).T * scale
    fz_high, fz_low = table_parts(forward_z)
    fz_all = np.concatenate([fz_high, fz_high, fz_low], axis=0)
    forward_y = np.concatenate([np.cos(angle_y.T), np.sin(angle_y.T)], axis=1) * scale
    member_x = np.arange(grid_side)
    wave_x = np.where(np.arange(M) < half, np.arange(M), np.arange(M) - M)
    angle_x = np.outer(wave_x, member_x) * step
    forward_x = np.concatenate([np.cos(angle_x), np.sin(angle_x)], axis=1) * scale
    inverse_x = np.concatenate([np.cos(angle_x.T), np.sin(angle_x.T)], axis=1) * M**-0.5
    lanes_y = np.broadcast_to(wave_y[:, None] + 2 * pair[None, :], (peers, 128))
    lanes_z = np.broadcast_to(wave_z[None, :], (peers, 128))
    return {
        "inverse_y": left_table(inverse_y),
        "turn_cos": turn_cos.astype(np.float32),
        "turn_sin": turn_sin.astype(np.float32),
        "iz_both": iz_both,
        "iz_high": iz_high,
        "fz_all": fz_all,
        "forward_y": left_table(forward_y),
        "forward_x": left_table(forward_x),
        "inverse_x": left_table(inverse_x),
        "lanes_y": lanes_y.astype(np.float32),
        "lanes_z": lanes_z.astype(np.float32),
        "wave_x": np.broadcast_to(wave_x[:, None], (M, 128)).astype(np.float32),
    }


def times_i(values):
    lane = lax.broadcasted_iota(jnp.int32, values.shape, 1)
    ahead = pltpu.roll(values, 96, 1)
    behind = pltpu.roll(values, 32, 1)
    return jnp.where(lane % 64 < 32, -ahead, behind)


def grid_kernel(arrived, iy, tc, ts, iz_both, iz_high, fz_all, fy, ly, lz, sent):
    wave_y, wave_z = ly[...], lz[...]
    turn_cos, turn_sin = tc[...], ts[...]
    for plane in range(planes):
        ux, uy, uz, dy, dz = [
            arrived[:, 0, (plane * 5 + k) * 128 : (plane * 5 + k + 1) * 128] for k in range(5)
        ]
        wx = times_i(wave_y * uz - wave_z * uy)
        wy = times_i(wave_z * ux) - dz
        wz = dy - times_i(wave_y * ux)
        packed = jnp.concatenate([ux, uy, uz, wx, wy, wz], axis=1)
        along_y = from_left(iy[...], packed)
        pieces = []
        for k in range(6):
            c = along_y[:grid_side, k * 128 : (k + 1) * 128]
            s = along_y[grid_side:, k * 128 : (k + 1) * 128]
            pieces.append(
                jnp.concatenate([turn_cos * c - turn_sin * s, turn_cos * s + turn_sin * c], axis=1)
            )
        high, low = two_parts(jnp.concatenate(pieces, axis=0))
        wide = jnp.dot(high, iz_both[...], preferred_element_type=jnp.float32)
        rest = jnp.dot(low, iz_high[...], preferred_element_type=jnp.float32)
        field = wide[:, :128] + wide[:, 128:] + rest
        f = [field[k * grid_side : (k + 1) * grid_side] for k in range(6)]
        product = jnp.concatenate(
            [
                f[1] * f[5] - f[2] * f[4],
                f[2] * f[3] - f[0] * f[5],
                f[0] * f[4] - f[1] * f[3],
            ],
            axis=0,
        )
        high, low = two_parts(product)
        along_z = jnp.dot(
            jnp.concatenate([high, low, high], axis=1), fz_all[...], preferred_element_type=jnp.float32
        )
        tops, lows = [], []
        for k in range(3):
            g = along_z[k * grid_side : (k + 1) * grid_side, :128]
            h = along_z[k * grid_side : (k + 1) * grid_side, 128:]
            tops.append(turn_cos * g + turn_sin * h)
            lows.append(turn_cos * h - turn_sin * g)
        stacked = jnp.concatenate(
            [jnp.concatenate(tops, axis=1), jnp.concatenate(lows, axis=1)], axis=0
        )
        result = from_left(fy[...], stacked)
        place = plane * 3 * 128
        sent[:, 0, place : place + 3 * 128] = result


def emit_modes(state, wave_x, table, sent):
    turned = [times_i(v) for v in state]
    top = state + [wave_x * turned[1], wave_x * turned[2]]
    low = turned + [-wave_x * state[1], -wave_x * state[2]]
    stacked = jnp.concatenate(
        [jnp.concatenate(top, axis=1), jnp.concatenate(low, axis=1)], axis=0
    )
    result = from_left(table, stacked)
    for plane in range(planes):
        sent[:, 0, plane * 640 : (plane + 1) * 640] = result[plane * peers : (plane + 1) * peers]


def start_kernel(state, wx, ix, sent):
    emit_modes([state[k] for k in range(3)], wx[...], ix[...], sent)


def modes_kernel(arrived, state, extra, wx, ly, lz, damp, gain, fx, ix, following, sent):
    fields = []
    for k in range(3):
        fields.append(
            jnp.concatenate(
                [
                    arrived[:, 0, (plane * 3 + k) * 128 : (plane * 3 + k + 1) * 128]
                    for plane in range(planes)
                ],
                axis=0,
            )
        )
    packed = jnp.concatenate(fields, axis=1)
    turned = jnp.concatenate([-times_i(v) for v in fields], axis=1)
    spectrum = from_left(fx[...], jnp.concatenate([packed, turned], axis=0))
    n = [spectrum[:, k * 128 : (k + 1) * 128] for k in range(3)]
    wave_x, wave_y, wave_z = wx[...], ly[...], lz[...]
    divergence = (wave_x * n[0] + wave_y * n[1] + wave_z * n[2]) * gain[...]
    waves = [wave_x, wave_y, wave_z]
    fresh = []
    for k in range(3):
        moved = state[k] + time_step * (n[k] - waves[k] * divergence)
        fresh.append(damp[...] * moved + extra[k])
        following[k] = fresh[k]
    emit_modes(fresh, wave_x, ix[...], sent)


def near(values):
    return pltpu.with_memory_space_constraint(values, pltpu.VMEM)


def chain_steps(place):
    tables = chain_tables()
    x, y, core = place
    wave_y = x * 16 + y * 4 + core
    wave_y = jnp.where(wave_y < M // 2, wave_y, wave_y - M)
    lane = jnp.arange(128, dtype=jnp.int32)
    lanes_y = (wave_y + lane // 64 * 2).astype(jnp.float32)[None, :]
    lanes_z = (lane % (M // 2)).astype(jnp.float32)[None, :]
    wave_x = jnp.asarray(tables["wave_x"])
    squared = wave_x * wave_x + lanes_y * lanes_y + lanes_z * lanes_z
    damp = jnp.exp(-viscosity * time_step * squared)
    gain = 1.0 / jnp.maximum(squared, 1.0)
    parcel = pltpu.VMEM((peers, 1, planes * 5 * 128), jnp.float32)
    shape = jax.ShapeDtypeStruct((3, M, 128), jnp.float32)
    dense = pltpu.VMEM((peers, 1, planes * 3 * 128), jnp.float32)
    grid_step = pl.pallas_call(grid_kernel, out_shape=dense, name="grid_step")
    modes_step = pl.pallas_call(modes_kernel, out_shape=(shape, parcel), name="modes_step")
    start_step = pl.pallas_call(start_kernel, out_shape=parcel, name="start_step")
    move = partial(lax.all_to_all, axis_name=ring, split_axis=0, concat_axis=0, tiled=True)
    grid_tables = [
        tables["inverse_y"],
        tables["turn_cos"],
        tables["turn_sin"],
        tables["iz_both"],
        tables["iz_high"],
        tables["fz_all"],
        tables["forward_y"],
        tables["lanes_y"],
        tables["lanes_z"],
    ]
    mode_tables = [
        wave_x, lanes_y, lanes_z, damp, gain, tables["forward_x"], tables["inverse_x"]
    ]

    def start(state):
        return start_step(state, wave_x, tables["inverse_x"])

    def grid_work(arrived):
        return grid_step(near(arrived), *grid_tables)

    def mode_work(arrived, state, extra):
        return modes_step(near(arrived), state, extra, *mode_tables)

    def follow(state, parcels, extra):
        return mode_work(move(grid_work(move(parcels))), state, extra)

    return start, follow, move, grid_work, mode_work


def chain_sweep(first, extras, place):
    start, follow = chain_steps(place)[:2]

    def turn(index, carried):
        state, parcels, history = carried
        extra = lax.dynamic_index_in_dim(extras, index, 0, keepdims=False)
        state, parcels = follow(state, parcels, extra)
        history = lax.dynamic_update_index_in_dim(history, state, index + 1, 0)
        return state, parcels, history

    history = jnp.zeros((16, 3, M, 128), jnp.float32)
    history = lax.dynamic_update_index_in_dim(history, first, 1, 0)
    return lax.fori_loop(1, 15, turn, (first, start(first), history))[2]


def to_ring(block, zh):
    pieces = jnp.moveaxis(block, 2, 0).reshape(4, 1, 3 * M // 2, 128)
    pieces = jnp.broadcast_to(pieces, (4, 2, 3 * M // 2, 128)).reshape(8, 3 * M // 2, 128)
    pieces = lax.all_to_all(pieces, ("x", "zh"), split_axis=0, concat_axis=0, tiled=True)
    pieces = lax.dynamic_slice_in_dim(pieces, zh * 4, 4, axis=0).reshape(2, 2, 3, M, M)
    return jnp.transpose(pieces, (0, 2, 3, 1, 4)).reshape(2, 3, M, 128)


def spread_payload(payload):
    copies = jnp.broadcast_to(payload.reshape(1, 6 * M, 128), (8, 6 * M, 128))
    gathered = lax.all_to_all(copies, ("zl", "zh"), split_axis=0, concat_axis=0, tiled=True)
    gathered = gathered.reshape(4, 2, 2, 3, M, 128)
    return jnp.transpose(gathered, (1, 2, 0, 3, 4, 5)).reshape(16, 3, M, 128)


def collect_slices(history, zl, zh):
    mine = lax.dynamic_index_in_dim(history.reshape(4, 4, 3, M, 2, M), zl, 1, keepdims=False)
    mine = lax.dynamic_index_in_dim(mine, zh, 3, keepdims=False)
    pieces = lax.all_to_all(
        mine.reshape(4, 3 * M // 2, 128), "x", split_axis=0, concat_axis=0, tiled=True
    )
    return jnp.moveaxis(pieces.reshape(4, 3, M, M), 0, 2)


def shards(start_states):
    x, zl, y, zh, core = [lax.axis_index(name) for name in ("x", "zl", "y", "zh", "core")]
    groups = 16
    member = (y * 2 + zh) * 2 + core
    layout = (4, 4, groups, member)
    place = (x, y, core)
    position = x * 4 + zl
    retained = start_states.shape[-1]
    stored = start_states.reshape(3, retained, start_states.shape[3], retained)
    spectral_state = project(stored, wave_grid(retained, layout))
    low_states = to_ring(restrict(spectral_state, M, groups), zh)
    fine_end, coarse_next = advance_both(spectral_state, low_states, place, layout)
    fine_low = restrict(fine_end, M, groups)
    low_ring = to_ring(fine_low, zh)
    opening = (zl == 0) & (zh == 0) & (jnp.arange(2) == 0)
    payload = jnp.where(opening[:, None, None, None], low_ring, low_ring - coarse_next)
    everything = spread_payload(payload)
    upper_band = jnp.where(shared_modes(retained, groups), 0.0, fine_end)
    previous = shifted(upper_band, ("x", "zl"), 1)
    history = chain_sweep(everything[0], everything, place)
    current = collect_slices(history, zl, zh)
    updated = prolong(current, retained, groups) + previous
    result = jnp.where(position == 0, spectral_state, updated)
    return result.reshape(1, result.shape[0], retained, result.shape[2], 1, retained)


def solution(mesh):
    split = Mesh(mesh.devices.reshape(4, 4, 4, 2, 2), ("x", "zl", "y", "zh", "core"))
    spec = P(("x", "zl"), None, None, None, ("y", "zh", "core"), None)
    return jax.shard_map(shards, mesh=split, in_specs=(spec,), out_specs=spec, check_vma=False)
```
